16 devices in a mesh: dp: 2 (over y, z), tp: 8 (over x, core).
Axes of the slice: x: 4, y: 2, z: 1, core: 2. Of those that a mesh axis runs over, the one named last changes fastest.
The devices are a block of a 4x4x4 slice.
Arguments:
- x: bfloat16 [128, 2048], P('dp'), parts along dimension 0
- k_cache: bfloat16 [128, 4096, 32, 64], P('dp', None, 'tp'), parts along dimension 0
- v_cache: bfloat16 [128, 4096, 32, 64], P('dp', None, 'tp'), parts along dimension 0
- gain_a: bfloat16 [2048], replicated
- wq: bfloat16 [2048, 2048], P(None, 'tp')
- wo: bfloat16 [2048, 2048], P('tp')
- gain_m: bfloat16 [2048], replicated
- w_gate: bfloat16 [2048, 5120], P(None, 'tp')
- w_up: bfloat16 [2048, 5120], P(None, 'tp')
- w_down: bfloat16 [5120, 2048], P('tp')
Outputs:
- output: bfloat16 [128, 2048], P('dp'), parts along dimension 0
There are 2 independent parts. The reference program is written for one: setup_inputs(seed, part) draws one part's arguments, and reference() takes and returns one part's arrays. A program takes and returns all parts, laid end to end along the dimension named above; an argument that names none is the same for every part.
All inputs are finite; a program needn't handle non-finite values.
Results may differ from the reference program's by a relative error of at most 0.017.
Values are sent between devices in bfloat16 or wider.
A program may use at most 1.5 GiB of HBM per device.

```python
import jax
import jax.numpy as jnp
from jax import lax

BATCH = 64
CACHE = 4096
D = 2048
HEADS = 32
KV_HEADS = 32
HEAD = 64
FF = 5120
THETA = 10000


def setup_inputs(seed: int = 0, part: int = 0) -> dict:
    kx, kc, kw, kn, kq, ko, km, kg, ku, kd = jax.random.split(jax.random.key(seed), 10)
    kx, kc, kw = (jax.random.fold_in(k, part) for k in (kx, kc, kw))

    def weights(key, rows, columns):
        return jax.random.normal(key, (rows, columns), jnp.float32) * rows**-0.5

    drawn = {
        "x": jax.random.normal(kx, (BATCH, D), jnp.float32),
        "k_cache": 2 * jax.random.normal(kc, (BATCH, CACHE, KV_HEADS, HEAD), jnp.float32),
        "v_cache": 4 * jax.random.normal(kw, (BATCH, CACHE, KV_HEADS, HEAD), jnp.float32),
        "gain_a": 1 + 0.1 * jax.random.normal(kn, (D,), jnp.float32),
        "wq": 2 * weights(kq, D, HEADS * HEAD),
        "wo": weights(ko, HEADS * HEAD, D),
        "gain_m": 1 + 0.1 * jax.random.normal(km, (D,), jnp.float32),
        "w_gate": weights(kg, D, FF),
        "w_up": weights(ku, D, FF),
        "w_down": 2 * weights(kd, FF, D),
    }
    return {k: v.astype(jnp.bfloat16) for k, v in drawn.items()}


def normed(x, gain):
    wide = x.astype(jnp.float32)
    scale = lax.rsqrt(jnp.mean(wide * wide, -1, keepdims=True) + 1e-6)
    return (wide * scale * gain.astype(jnp.float32)).astype(jnp.bfloat16)


def turned(t, place, theta):
    half = t.shape[-1] // 2
    angle = place.astype(jnp.float32)[:, None] * theta ** (-jnp.arange(half, dtype=jnp.float32) / half)
    cos, sin = jnp.cos(angle)[:, None], jnp.sin(angle)[:, None]
    a, b = t[..., :half].astype(jnp.float32), t[..., half:].astype(jnp.float32)
    return jnp.concatenate([a * cos - b * sin, b * cos + a * sin], -1).astype(jnp.bfloat16)


def matmul(a, w):
    return jnp.dot(a, w, preferred_element_type=jnp.float32).astype(jnp.bfloat16)


def einsum(form, a, b):
    return jnp.einsum(form, a.astype(jnp.float32), b.astype(jnp.float32))


def seen_by(a, wq, k_cache, v_cache, head, theta):
    batch, cache, kv_heads = k_cache.shape[:3]
    place = jnp.full((batch,), cache - 1)
    q = turned(matmul(a, wq).reshape(batch, -1, head), place, theta).reshape(batch, kv_heads, -1, head)
    scores = einsum("bgsd,bugd->bgsu", q, k_cache) * head**-0.5
    weights = jax.nn.softmax(scores, -1).astype(jnp.bfloat16)
    return einsum("bgsu,bugd->bgsd", weights, v_cache).astype(jnp.bfloat16).reshape(batch, -1)


def hidden_of(b, w_gate, w_up):
    gate = jnp.dot(b, w_gate, preferred_element_type=jnp.float32)
    up = jnp.dot(b, w_up, preferred_element_type=jnp.float32)
    return (jax.nn.silu(gate) * up).astype(jnp.bfloat16)


def reference(x, k_cache, v_cache, gain_a, wq, wo, gain_m, w_gate, w_up, w_down):
    seen = seen_by(normed(x, gain_a), wq, k_cache, v_cache, HEAD, THETA)
    h = (x.astype(jnp.float32) + jnp.dot(seen, wo, preferred_element_type=jnp.float32)).astype(jnp.bfloat16)
    hidden = hidden_of(normed(h, gain_m), w_gate, w_up)
    return (h.astype(jnp.float32) + jnp.dot(hidden, w_down, preferred_element_type=jnp.float32)).astype(jnp.bfloat16)
```

```python
import functools
import math

import jax
import jax.numpy as jnp
import numpy as np
from jax import lax
from jax.experimental import pallas as pl
from jax.experimental.pallas import tpu as pltpu
from jax.sharding import PartitionSpec as P

HEAD = 64
THETA = 10000
MESH = pl.DeviceIdType.MESH

SLOTS = 4
EARLY = 2
CHUNKS = ((52, (0, 4, 8, 12.1, 16.1)), (8, (0, 4.2, 8.2)), (4, (0, 4, 8)))
ROWS = 8
LANES = 128


def turns(heads, place):
    half = HEAD // 2
    angle = np.float32(place) * np.float32(THETA) ** (-np.arange(half, dtype=np.float32) / np.float32(half))
    angle = angle.astype(np.float64)
    cos, sin = np.cos(angle), np.sin(angle)
    own, other = np.concatenate([cos, cos]), np.concatenate([-sin, sin])
    return np.stack([np.tile(own, heads), np.tile(other, heads)]).astype(np.float32)


def scaled(wide, gain):
    scale = lax.rsqrt(jnp.mean(wide * wide, -1, keepdims=True) + 1e-6)
    return (wide * scale * gain).astype(jnp.bfloat16)


def blocks(rows):
    return [(r, min(ROWS, rows - r)) for r in range(0, rows, ROWS)]


def added(parts):
    while len(parts) > 1:
        parts = [a + b for a, b in zip(parts[::2], parts[1::2])] + parts[len(parts) & ~1:]
    return parts[0]


def kernel(n, chunks, x_hbm, k_hbm, v_hbm, ga_hbm, wq_hbm, wo_hbm, gm_hbm, wg_hbm, wu_hbm, wd_hbm, turn_hbm, y_hbm,
           x, ga, wq, wo, gm, wg, wu, wd, turn, kbuf, vbuf, query, weights, seen, normal, y,
           terms, parts, h, sums, first_sem, later_sem, ksem, vsem, ysem, send_sem, recv_sem):
    batch, d = x.shape
    width = wq.shape[1]
    share = d // n
    me = lax.axis_index("tp")
    mine = pl.ds(pl.multiple_of(me * share, share), share)
    row_of = lax.broadcasted_iota(jnp.int32, (ROWS, width), 0)
    head_of = lax.broadcasted_iota(jnp.int32, (ROWS, width), 1) // HEAD
    own = row_of == head_of

    first = [pltpu.make_async_copy(a, b, first_sem.at[i])
             for i, (a, b) in enumerate(((x_hbm, x), (ga_hbm, ga), (turn_hbm, turn), (wq_hbm, wq)))]
    later = [pltpu.make_async_copy(a, b, later_sem.at[i])
             for i, (a, b) in enumerate(((wo_hbm, wo), (gm_hbm, gm), (wg_hbm, wg), (wu_hbm, wu), (wd_hbm, wd)))]

    def keys(i):
        slot = lax.rem(i, SLOTS)
        return pltpu.make_async_copy(k_hbm.at[i], kbuf.at[slot], ksem.at[slot])

    def values(i):
        slot = lax.rem(i, SLOTS)
        return pltpu.make_async_copy(v_hbm.at[i], vbuf.at[slot], vsem.at[slot])

    def peer(k):
        return lax.rem(me + k, n)

    def remote(step, c, k, source, target):
        return pltpu.make_async_remote_copy(
            src_ref=source, dst_ref=target, send_sem=send_sem.at[step, c, k - 1], recv_sem=recv_sem.at[step, c, k - 1],
            device_id={"tp": peer(k)}, device_id_type=MESH)

    def start(copies):
        for copy in copies:
            copy.start()

    def wait(copies):
        for copy in copies:
            copy.wait_send()
            copy.wait_recv()

    def wide_gain(g):
        g = g[...].astype(jnp.float32)
        return jnp.concatenate([g[i:i + 1] for i in range(g.shape[0])], 1)

    def attend_keys(i):
        slot = lax.rem(i, SLOTS)
        q = jnp.where(own, jnp.broadcast_to(query[pl.ds(i, 1), :], (ROWS, width)), 0.0).astype(jnp.bfloat16)
        scores = jnp.dot(q, kbuf[slot], preferred_element_type=jnp.float32)
        top = jnp.max(scores, -1, keepdims=True)
        p = jnp.exp2((scores - top) * (HEAD**-0.5 * math.log2(math.e)))
        p = p * (1.0 / jnp.sum(p, -1, keepdims=True))
        return p.astype(jnp.bfloat16)

    def attend_values(i, w):
        slot = lax.rem(i, SLOTS)
        o = lax.dot_general(w, vbuf[slot], (((1,), (1,)), ((), ())), preferred_element_type=jnp.float32)
        o = jnp.sum(jnp.where(own, o, 0.0), 0, keepdims=True)
        seen[pl.ds(i, 1), :] = o

    def attended(c):
        at, rows, _ = chunks[c]
        return jnp.dot(seen[pl.ds(at, rows), :].astype(jnp.bfloat16), wo[...], preferred_element_type=jnp.float32).astype(jnp.bfloat16)

    def fed(b):
        gate = jnp.dot(b, wg[...], preferred_element_type=jnp.float32)
        up = jnp.dot(b, wu[...], preferred_element_type=jnp.float32)
        hidden = (jax.nn.silu(gate) * up).astype(jnp.bfloat16)
        return jnp.dot(hidden, wd[...], preferred_element_type=jnp.float32).astype(jnp.bfloat16)

    def y_copy(c):
        at, rows, _ = chunks[c]
        on = pl.ds(at // ROWS * ROWS, (at + rows) // ROWS * ROWS - at // ROWS * ROWS)
        return None

    def scatter(half, c):
        return [remote(2 * half, c, k, terms[c].at[half, :, pl.ds(pl.multiple_of(peer(k) * share, share), share)],
                       parts[c].at[half, k - 1]) for k in range(1, n)]

    def gather(half, c):
        block = (h, sums)[half][c].at[:, mine]
        return [remote(2 * half + 1, c, k, block, block) for k in range(1, n)]

    def scattered(half, c, value):
        terms[c][half] = value
        start(scatter(half, c))

    def reduced(half, c):
        wait(scatter(half, c))
        at, rows, _ = chunks[c]
        for r, m in blocks(rows):
            on = pl.ds(r, m)
            total = added([terms[c][half, on, mine].astype(jnp.float32)]
                          + [parts[c][half, k, on, :].astype(jnp.float32) for k in range(n - 1)])
            t = h[c][on, mine] if half else x[pl.ds(at + r, m), mine]
            (h, sums)[half][c][on, mine] = (t.astype(jnp.float32) + total).astype(jnp.bfloat16)
        start(gather(half, c))

    def project(c):
        scattered(0, c, attended(c))

    def feed(c):
        wait(gather(0, c))
        at, rows, _ = chunks[c]
        gain = wide_gain(gm)
        for r, m in blocks(rows):
            normal[pl.ds(r, m), :] = scaled(h[c][pl.ds(r, m), :].astype(jnp.float32), gain)
        scattered(1, c, fed(normal[pl.ds(0, rows), :]))

    def finish(c):
        wait(gather(1, c))
        at, rows, _ = chunks[c]
        y_hbm[pl.ds(at, rows), :] = sums[c][...]
        pass

    def shout(half, c):
        return [remote(2 * half, c, k, terms[c].at[half], parts[c].at[half, me]) for k in range(1, n)]

    def shouted(half, c, value):
        terms[c][half] = value
        parts[c][half, me] = value
        start(shout(half, c))

    def heard(half, c, t):
        wait(shout(half, c))
        total = added([parts[c][half, s].astype(jnp.float32) for s in range(n)])
        return (t.astype(jnp.float32) + total).astype(jnp.bfloat16)

    def small_project(c):
        shouted(0, c, attended(c))

    def small_feed(c):
        at, rows, _ = chunks[c]
        now = heard(0, c, x[pl.ds(at, rows), :])
        h[c][...] = now
        shouted(1, c, fed(scaled(now.astype(jnp.float32), wide_gain(gm))))

    def small_finish(c):
        at, rows, _ = chunks[c]
        y_hbm[pl.ds(at, rows), :] = heard(1, c, h[c][...])
        pass

    start(first)
    keys(0).start()
    for i in range(1, EARLY):
        keys(i).start()
        values(i - 1).start()
    barrier = pltpu.get_barrier_semaphore()
    for k in range(1, n):
        pl.semaphore_signal(barrier, inc=1, device_id={"tp": peer(k)}, device_id_type=MESH)

    for copy in first:
        copy.wait()
    for i in range(EARLY, SLOTS):
        keys(i).start()
        values(i - 1).start()
    values(SLOTS - 1).start()
    gain = wide_gain(ga)
    for r, m in blocks(batch):
        normal[pl.ds(r, m), :] = scaled(x[pl.ds(r, m), :].astype(jnp.float32), gain)
    q = jnp.dot(normal[...], wq[...], preferred_element_type=jnp.float32).astype(jnp.bfloat16).astype(jnp.float32)
    lane = lax.broadcasted_iota(jnp.int32, q.shape, 1)
    other = jnp.where(lane % HEAD < HEAD // 2, pltpu.roll(q, width - HEAD // 2, 1), pltpu.roll(q, HEAD // 2, 1))
    query[...] = (q * turn[0:1, :] + other * turn[1:2, :]).astype(jnp.bfloat16).astype(jnp.float32)

    pl.semaphore_wait(barrier, n - 1)

    steps = []
    for c, (at, rows, offsets) in enumerate(chunks):
        each = (small_project, small_feed, small_finish)
        if len(offsets) > len(each):
            each = (project, functools.partial(reduced, 0), feed, functools.partial(reduced, 1), finish)
        steps += [(at + rows + offset, functools.partial(f, c)) for offset, f in zip(offsets, each)]
    steps.sort(key=lambda step: step[0])
    events = {}
    for at, f in steps:
        if math.ceil(at) < batch:
            events.setdefault(math.ceil(at), []).append(f)

    keys(0).wait()
    weights[...] = attend_keys(0)
    keys(SLOTS).start()

    @pl.loop(1, batch)
    def _(i):
        keys(i).wait()
        values(i - 1).wait()
        attend_values(i - 1, weights[...])
        weights[...] = attend_keys(i)

        @pl.when(i + SLOTS < batch)
        def _():
            keys(i + SLOTS).start()

        @pl.when(i - 1 + SLOTS < batch)
        def _():
            values(i - 1 + SLOTS).start()

        @pl.when(i == 8)
        def _():
            start(later)

        @pl.when(i == 16)
        def _():
            for copy in later:
                copy.wait()

        for at, what in events.items():
            @pl.when(i == at)
            def _():
                for f in what:
                    f()

    values(batch - 1).wait()
    attend_values(batch - 1, weights[...])
    for at, f in steps:
        if math.ceil(at) >= batch:
            f()
    for c in range(len(chunks)):
        pass


def solution(mesh):
    n = mesh.shape["tp"]

    def step(x, k_cache, v_cache, gain_a, wq, wo, gain_m, w_gate, w_up, w_down):
        batch, cache, heads, head = k_cache.shape
        d, width, hidden = x.shape[1], wq.shape[1], w_gate.shape[1]
        chunks, at = [], 0
        for rows, offsets in CHUNKS:
            chunks.append((at, rows, offsets))
            at += rows
        assert at == batch
        flat = lambda t: jnp.transpose(t, (0, 2, 3, 1)).reshape(batch, heads * head, cache)
        bf16, f32 = jnp.bfloat16, jnp.float32
        operands = (x, flat(k_cache), flat(v_cache), gain_a.reshape(-1, LANES), wq, wo, gain_m.reshape(-1, LANES), w_gate, w_up, w_down,
                    jnp.asarray(turns(heads, cache - 1)))
        scratch = [
            pltpu.VMEM((batch, d), bf16), pltpu.VMEM((d // LANES, LANES), bf16), pltpu.VMEM(wq.shape, bf16), pltpu.VMEM(wo.shape, bf16),
            pltpu.VMEM((d // LANES, LANES), bf16), pltpu.VMEM(w_gate.shape, bf16), pltpu.VMEM(w_up.shape, bf16), pltpu.VMEM(w_down.shape, bf16),
            pltpu.VMEM((2, width), f32),
            pltpu.VMEM((SLOTS, width, cache), bf16), pltpu.VMEM((SLOTS, width, cache), bf16),
            pltpu.VMEM((batch, width), f32), pltpu.VMEM((ROWS, cache), bf16), pltpu.VMEM((batch, width), f32),
            pltpu.VMEM((batch, d), bf16), pltpu.VMEM((batch, d), bf16),
            [pltpu.VMEM((2, r, d), bf16) for _, r, _ in chunks],
            [pltpu.VMEM((2, n, r, d), bf16) if len(o) < 5 else pltpu.VMEM((2, n - 1, r, d // n), bf16) for _, r, o in chunks],
            [pltpu.VMEM((r, d), bf16) for _, r, _ in chunks], [pltpu.VMEM((r, d), bf16) for _, r, _ in chunks],
            pltpu.SemaphoreType.DMA((4,)), pltpu.SemaphoreType.DMA((5,)),
            pltpu.SemaphoreType.DMA((SLOTS,)), pltpu.SemaphoreType.DMA((SLOTS,)), pltpu.SemaphoreType.DMA((len(chunks),)),
            pltpu.SemaphoreType.DMA((4, len(chunks), n - 1)), pltpu.SemaphoreType.DMA((4, len(chunks), n - 1)),
        ]
        return pl.pallas_call(
            functools.partial(kernel, n, chunks),
            out_shape=pltpu.VMEM((batch, d), bf16),
            in_specs=[pl.BlockSpec(memory_space=pl.ANY)] * len(operands),
            out_specs=pl.BlockSpec(memory_space=pltpu.VMEM),
            scratch_shapes=scratch,
            compiler_params=pltpu.CompilerParams(collective_id=0, has_side_effects=True, vmem_limit_bytes=56 * 2**20),
            cost_estimate=pl.CostEstimate(flops=2 * batch * width * cache * 4, bytes_accessed=4 * batch * width * cache, transcendentals=0),
            name="layer",
        )(*operands)

    states, cache, columns, rows_of = P("dp", None), P("dp", None, "tp", None), P(None, "tp"), P("tp", None)
    return jax.shard_map(
        step,
        mesh=mesh,
        in_specs=(states, cache, cache, P(None), columns, rows_of, P(None), columns, columns, rows_of),
        out_specs=states,
        check_vma=False,
    )
```

```python
import functools
import math

import jax
import jax.numpy as jnp
import numpy as np
from jax import lax
from jax.experimental import pallas as pl
from jax.experimental.pallas import tpu as pltpu
from jax.sharding import PartitionSpec as P

HEAD = 64
THETA = 10000
MESH = pl.DeviceIdType.MESH

SLOTS = 4
EARLY = 2
CHUNKS = ((52, (0, 4, 8, 12.1, 16.1)), (8, (0, 4.2, 8.2)), (4, (0, 4, 8)))
ROWS = 8
LANES = 128


def turns(heads, place):
    half = HEAD // 2
    angle = np.float32(place) * np.float32(THETA) ** (-np.arange(half, dtype=np.float32) / np.float32(half))
    angle = angle.astype(np.float64)
    cos, sin = np.cos(angle), np.sin(angle)
    own, other = np.concatenate([cos, cos]), np.concatenate([-sin, sin])
    return np.stack([np.tile(own, heads), np.tile(other, heads)]).astype(np.float32)


def scaled(wide, gain):
    scale = lax.rsqrt(jnp.mean(wide * wide, -1, keepdims=True) + 1e-6)
    return (wide * scale * gain).astype(jnp.bfloat16)


def blocks(rows):
    return [(r, min(ROWS, rows - r)) for r in range(0, rows, ROWS)]


def added(parts):
    while len(parts) > 1:
        parts = [a + b for a, b in zip(parts[::2], parts[1::2])] + parts[len(parts) & ~1:]
    return parts[0]


def kernel(n, chunks, x_hbm, k_hbm, v_hbm, ga_hbm, wq_hbm, wo_hbm, gm_hbm, wg_hbm, wu_hbm, wd_hbm, turn_hbm, y_hbm,
           x, ga, wq, wo, gm, wg, wu, wd, turn, kbuf, vbuf, query, weights, seen, normal, y,
           terms, parts, h, sums, first_sem, later_sem, ksem, vsem, ysem, send_sem, recv_sem):
    batch, d = x.shape
    width = wq.shape[1]
    share = d // n
    others = sorted(range(1, n), key=lambda k: abs(n - 2 * k))
    me = lax.axis_index("tp")
    mine = pl.ds(pl.multiple_of(me * share, share), share)
    row_of = lax.broadcasted_iota(jnp.int32, (ROWS, width), 0)
    head_of = lax.broadcasted_iota(jnp.int32, (ROWS, width), 1) // HEAD
    own = row_of == head_of

    first = [pltpu.make_async_copy(a, b, first_sem.at[i])
             for i, (a, b) in enumerate(((x_hbm, x), (ga_hbm, ga), (turn_hbm, turn), (wq_hbm, wq)))]
    later = [pltpu.make_async_copy(a, b, later_sem.at[i])
             for i, (a, b) in enumerate(((wo_hbm, wo), (gm_hbm, gm), (wg_hbm, wg), (wu_hbm, wu), (wd_hbm, wd)))]

    def keys(i):
        slot = lax.rem(i, SLOTS)
        return pltpu.make_async_copy(k_hbm.at[i], kbuf.at[slot], ksem.at[slot])

    def values(i):
        slot = lax.rem(i, SLOTS)
        return pltpu.make_async_copy(v_hbm.at[i], vbuf.at[slot], vsem.at[slot])

    def peer(k):
        return lax.rem(me + k, n)

    def remote(step, c, k, source, target):
        return pltpu.make_async_remote_copy(
            src_ref=source, dst_ref=target, send_sem=send_sem.at[step, c, k - 1], recv_sem=recv_sem.at[step, c, k - 1],
            device_id={"tp": peer(k)}, device_id_type=MESH)

    def start(copies):
        for copy in copies:
            copy.start()

    def wait(copies):
        for copy in copies:
            copy.wait_send()
            copy.wait_recv()

    def wide_gain(g):
        g = g[...].astype(jnp.float32)
        return jnp.concatenate([g[i:i + 1] for i in range(g.shape[0])], 1)

    def attend_keys(i):
        slot = lax.rem(i, SLOTS)
        q = jnp.where(own, jnp.broadcast_to(query[pl.ds(i, 1), :], (ROWS, width)), 0.0).astype(jnp.bfloat16)
        scores = jnp.dot(q, kbuf[slot], preferred_element_type=jnp.float32)
        top = jnp.max(scores, -1, keepdims=True)
        p = jnp.exp2((scores - top) * (HEAD**-0.5 * math.log2(math.e)))
        p = p * (1.0 / jnp.sum(p, -1, keepdims=True))
        return p.astype(jnp.bfloat16)

    def attend_values(i, w):
        slot = lax.rem(i, SLOTS)
        o = lax.dot_general(w, vbuf[slot], (((1,), (1,)), ((), ())), preferred_element_type=jnp.float32)
        o = jnp.sum(jnp.where(own, o, 0.0), 0, keepdims=True)
        seen[pl.ds(i, 1), :] = o

    def attended(c):
        at, rows, _ = chunks[c]
        return jnp.dot(seen[pl.ds(at, rows), :].astype(jnp.bfloat16), wo[...], preferred_element_type=jnp.float32).astype(jnp.bfloat16)

    def fed(b):
        gate = jnp.dot(b, wg[...], preferred_element_type=jnp.float32)
        up = jnp.dot(b, wu[...], preferred_element_type=jnp.float32)
        hidden = (jax.nn.silu(gate) * up).astype(jnp.bfloat16)
        return jnp.dot(hidden, wd[...], preferred_element_type=jnp.float32).astype(jnp.bfloat16)

    def y_copy(c):
        at, rows, _ = chunks[c]
        on = pl.ds(at // ROWS * ROWS, (at + rows) // ROWS * ROWS - at // ROWS * ROWS)
        return None

    def scatter(half, c):
        return [remote(2 * half, c, k, terms[c].at[half, :, pl.ds(pl.multiple_of(peer(k) * share, share), share)],
                       parts[c].at[half, k - 1]) for k in others]

    def gather(half, c):
        block = (h, sums)[half][c].at[:, mine]
        return [remote(2 * half + 1, c, k, block, block) for k in others]

    def scattered(half, c, value):
        terms[c][half] = value
        start(scatter(half, c))

    def reduced(half, c):
        wait(scatter(half, c))
        at, rows, _ = chunks[c]
        for r, m in blocks(rows):
            on = pl.ds(r, m)
            total = added([terms[c][half, on, mine].astype(jnp.float32)]
                          + [parts[c][half, k, on, :].astype(jnp.float32) for k in range(n - 1)])
            t = h[c][on, mine] if half else x[pl.ds(at + r, m), mine]
            (h, sums)[half][c][on, mine] = (t.astype(jnp.float32) + total).astype(jnp.bfloat16)
        start(gather(half, c))

    def project(c):
        scattered(0, c, attended(c))

    def feed(c):
        wait(gather(0, c))
        at, rows, _ = chunks[c]
        gain = wide_gain(gm)
        for r, m in blocks(rows):
            normal[pl.ds(r, m), :] = scaled(h[c][pl.ds(r, m), :].astype(jnp.float32), gain)
        scattered(1, c, fed(normal[pl.ds(0, rows), :]))

    def finish(c):
        wait(gather(1, c))
        at, rows, _ = chunks[c]
        y_hbm[pl.ds(at, rows), :] = sums[c][...]
        pass

    def shout(half, c):
        return [remote(2 * half, c, k, terms[c].at[half], parts[c].at[half, me]) for k in others]

    def shouted(half, c, value):
        terms[c][half] = value
        parts[c][half, me] = value
        start(shout(half, c))

    def heard(half, c, t):
        wait(shout(half, c))
        total = added([parts[c][half, s].astype(jnp.float32) for s in range(n)])
        return (t.astype(jnp.float32) + total).astype(jnp.bfloat16)

    def small_project(c):
        shouted(0, c, attended(c))

    def small_feed(c):
        at, rows, _ = chunks[c]
        now = heard(0, c, x[pl.ds(at, rows), :])
        h[c][...] = now
        shouted(1, c, fed(scaled(now.astype(jnp.float32), wide_gain(gm))))

    def small_finish(c):
        at, rows, _ = chunks[c]
        y_hbm[pl.ds(at, rows), :] = heard(1, c, h[c][...])
        pass

    start(first)
    keys(0).start()
    for i in range(1, EARLY):
        keys(i).start()
        values(i - 1).start()
    barrier = pltpu.get_barrier_semaphore()
    for k in range(1, n):
        pl.semaphore_signal(barrier, inc=1, device_id={"tp": peer(k)}, device_id_type=MESH)

    for copy in first:
        copy.wait()
    for i in range(EARLY, SLOTS):
        keys(i).start()
        values(i - 1).start()
    values(SLOTS - 1).start()
    gain = wide_gain(ga)
    for r, m in blocks(batch):
        normal[pl.ds(r, m), :] = scaled(x[pl.ds(r, m), :].astype(jnp.float32), gain)
    q = jnp.dot(normal[...], wq[...], preferred_element_type=jnp.float32).astype(jnp.bfloat16).astype(jnp.float32)
    lane = lax.broadcasted_iota(jnp.int32, q.shape, 1)
    other = jnp.where(lane % HEAD < HEAD // 2, pltpu.roll(q, width - HEAD // 2, 1), pltpu.roll(q, HEAD // 2, 1))
    query[...] = (q * turn[0:1, :] + other * turn[1:2, :]).astype(jnp.bfloat16).astype(jnp.float32)

    pl.semaphore_wait(barrier, n - 1)

    steps = []
    for c, (at, rows, offsets) in enumerate(chunks):
        each = (small_project, small_feed, small_finish)
        if len(offsets) > len(each):
            each = (project, functools.partial(reduced, 0), feed, functools.partial(reduced, 1), finish)
        steps += [(at + rows + offset, functools.partial(f, c)) for offset, f in zip(offsets, each)]
    steps.sort(key=lambda step: step[0])
    events = {}
    for at, f in steps:
        if math.ceil(at) < batch:
            events.setdefault(math.ceil(at), []).append(f)

    keys(0).wait()
    weights[...] = attend_keys(0)
    keys(SLOTS).start()

    @pl.loop(1, batch)
    def _(i):
        keys(i).wait()
        values(i - 1).wait()
        old = weights[...]
        new = attend_keys(i)
        attend_values(i - 1, old)
        weights[...] = new

        @pl.when(i + SLOTS < batch)
        def _():
            keys(i + SLOTS).start()

        @pl.when(i - 1 + SLOTS < batch)
        def _():
            values(i - 1 + SLOTS).start()

        @pl.when(i == 8)
        def _():
            start(later)

        @pl.when(i == 16)
        def _():
            for copy in later:
                copy.wait()

        for at, what in events.items():
            @pl.when(i == at)
            def _():
                for f in what:
                    f()

    values(batch - 1).wait()
    attend_values(batch - 1, weights[...])
    for at, f in steps:
        if math.ceil(at) >= batch:
            f()
    for c in range(len(chunks)):
        pass


def solution(mesh):
    n = mesh.shape["tp"]

    def step(x, k_cache, v_cache, gain_a, wq, wo, gain_m, w_gate, w_up, w_down):
        batch, cache, heads, head = k_cache.shape
        d, width, hidden = x.shape[1], wq.shape[1], w_gate.shape[1]
        chunks, at = [], 0
        for rows, offsets in CHUNKS:
            chunks.append((at, rows, offsets))
            at += rows
        assert at == batch
        flat = lambda t: jnp.transpose(t, (0, 2, 3, 1)).reshape(batch, heads * head, cache)
        bf16, f32 = jnp.bfloat16, jnp.float32
        operands = (x, flat(k_cache), flat(v_cache), gain_a.reshape(-1, LANES), wq, wo, gain_m.reshape(-1, LANES), w_gate, w_up, w_down,
                    jnp.asarray(turns(heads, cache - 1)))
        scratch = [
            pltpu.VMEM((batch, d), bf16), pltpu.VMEM((d // LANES, LANES), bf16), pltpu.VMEM(wq.shape, bf16), pltpu.VMEM(wo.shape, bf16),
            pltpu.VMEM((d // LANES, LANES), bf16), pltpu.VMEM(w_gate.shape, bf16), pltpu.VMEM(w_up.shape, bf16), pltpu.VMEM(w_down.shape, bf16),
            pltpu.VMEM((2, width), f32),
            pltpu.VMEM((SLOTS, width, cache), bf16), pltpu.VMEM((SLOTS, width, cache), bf16),
            pltpu.VMEM((batch, width), f32), pltpu.VMEM((ROWS, cache), bf16), pltpu.VMEM((batch, width), f32),
            pltpu.VMEM((batch, d), bf16), pltpu.VMEM((batch, d), bf16),
            [pltpu.VMEM((2, r, d), bf16) for _, r, _ in chunks],
            [pltpu.VMEM((2, n, r, d), bf16) if len(o) < 5 else pltpu.VMEM((2, n - 1, r, d // n), bf16) for _, r, o in chunks],
            [pltpu.VMEM((r, d), bf16) for _, r, _ in chunks], [pltpu.VMEM((r, d), bf16) for _, r, _ in chunks],
            pltpu.SemaphoreType.DMA((4,)), pltpu.SemaphoreType.DMA((5,)),
            pltpu.SemaphoreType.DMA((SLOTS,)), pltpu.SemaphoreType.DMA((SLOTS,)), pltpu.SemaphoreType.DMA((len(chunks),)),
            pltpu.SemaphoreType.DMA((4, len(chunks), n - 1)), pltpu.SemaphoreType.DMA((4, len(chunks), n - 1)),
        ]
        return pl.pallas_call(
            functools.partial(kernel, n, chunks),
            out_shape=pltpu.VMEM((batch, d), bf16),
            in_specs=[pl.BlockSpec(memory_space=pl.ANY)] * len(operands),
            out_specs=pl.BlockSpec(memory_space=pltpu.VMEM),
            scratch_shapes=scratch,
            compiler_params=pltpu.CompilerParams(collective_id=0, has_side_effects=True, vmem_limit_bytes=56 * 2**20),
            cost_estimate=pl.CostEstimate(flops=2 * batch * width * cache * 4, bytes_accessed=4 * batch * width * cache, transcendentals=0),
            name="layer",
        )(*operands)

    states, cache, columns, rows_of = P("dp", None), P("dp", None, "tp", None), P(None, "tp"), P("tp", None)
    return jax.shard_map(
        step,
        mesh=mesh,
        in_specs=(states, cache, cache, P(None), columns, rows_of, P(None), columns, columns, rows_of),
        out_specs=states,
        check_vma=False,
    )
```
